32 devices in a mesh: groups: 2 (over x), expert: 16 (over z, y, core).
Axes of the slice: x: 2, y: 2, z: 4, core: 2. Of those that a mesh axis runs over, the one named last changes fastest.
Arguments:
- tokens: bfloat16 [4096, 7168], P(('groups', 'expert')), parts along dimension 0, may hold values from -6 to 6
- route_ids: int32 [4096, 2], P(('groups', 'expert')), parts along dimension 0, may hold values from 0 to 3, all different within a row; in each aligned block of 128 rows (0 to 127, 128 to 255, ...) at most 80 rows name the same one
- levels: int32 [4096, 2], P(('groups', 'expert')), parts along dimension 0, may hold values from 1 to 64
- w_gate: bfloat16 [16, 7168, 512], P('expert'), may hold values from -0.0625 to 0.0625
- w_up: bfloat16 [16, 7168, 512], P('expert'), may hold values from -0.0625 to 0.0625
- w_down: bfloat16 [16, 512, 7168], P('expert'), may hold values from -0.125 to 0.125
Outputs:
- combined: bfloat16 [4096, 7168], P(('groups', 'expert')), parts along dimension 0
The draws below stay inside these ranges and needn't reach their ends.
There are 2 independent parts, one for each index of `groups`. The reference program is written for one: setup_inputs(seed, part) draws one part's arguments, and reference() takes and returns one part's arrays. A program takes and returns all parts, laid end to end along the dimension named above; an argument that names none is the same for every part. Nothing has to cross between parts.
Inputs may be any that keep to these rules, and one draw needn't show every extreme that they name: `route_ids`: each row names 2 different experts; among the rows of one device no expert is named more than 80 times, a bound that some block reaches.
All inputs are finite; a program needn't handle non-finite values.
Results may differ from the reference program's by a relative error of at most 0.013.
Values may be sent and summed in bfloat16 or wider, within the bound.
A program may use at most 192 MiB of HBM per device.

```python
import math
import jax
import jax.numpy as jnp
import numpy as np
from jax import lax

D = 7168
FF_WIN = 2048
SHARDS = 4
FF_DEV = 512
TOK_DEV = 128
TOP = 2
EXPERTS = 4
CAP = 80
TOKENS = 2048
N_EXPERT = 16


def set_ends(values, rng, smallest, high):
    spot = [jax.random.randint(jax.random.fold_in(rng, axis), (), 0, length) for axis, length in enumerate(values.shape)]
    longest = values.shape.index(max(values.shape))
    neighbour = spot[:longest] + [(spot[longest] + 1) % values.shape[longest]] + spot[longest + 1:]
    return values.at[tuple(spot)].set(smallest).at[tuple(neighbour)].set(high)


def steps_of(own_key, extent, split, low, high):
    level, own = 1.0, jax.random.fold_in(own_key, 6)
    for position, shards_of in split:
        heights = jnp.exp(jax.random.uniform(jax.random.fold_in(own, position), (shards_of,), jnp.float32, low / len(split), high / len(split)))
        level = level * jnp.repeat(heights, extent[position] // shards_of).reshape([-1 if axis == position else 1 for axis in range(len(extent))])
    return level


def shared_out(key, own, number, rows, count, top, limit, slope):
    sequence = jax.random.permutation(key, count)
    packed, usual = portions_of(count, rows * top, limit, slope, True), portions_of(count, rows * top, limit, slope, False)
    places = jnp.arange(count)

    def named(tallies, offset_by):
        used = int((tallies > 0).sum())
        fixed = max(1, used // 4)
        shifted = fixed + (places - fixed + offset_by * (used - fixed)) % max(1, count - fixed)
        return jnp.zeros((count,), jnp.int32).at[sequence[jnp.where(places < fixed, places, shifted)]].set(jnp.asarray(tallies, jnp.int32))

    tallies = jnp.where(number % 4 == 0, named(packed, number // 4), named(usual, number - number // 4 - 1))
    mixed = jax.random.permutation(jax.random.fold_in(own, 3), count)
    donor, sink = mixed[0:count // 2 * 2:2], mixed[1:count // 2 * 2:2]
    margin = jnp.minimum(tallies[donor] - 1, limit - tallies[sink]) // 2
    margin = jnp.where((donor == sequence[0]) | (sink == sequence[0]) | (tallies[sink] == 0), 0, jnp.maximum(margin, 0))
    shifted = jax.random.randint(jax.random.fold_in(own, 4), (count // 2,), 0, 1 << 20) % (margin + 1)
    tallies = tallies.at[donor].add(-shifted).at[sink].add(shifted)
    members = jnp.searchsorted(jnp.cumsum(tallies), jnp.arange(rows * top), side="right").astype(jnp.int32)
    table = members.reshape(top, rows).T
    table = table[jax.random.permutation(jax.random.fold_in(own, 1), rows)]
    offset_by = jax.random.randint(jax.random.fold_in(own, 2), (rows, 1), 0, top)
    return jnp.take_along_axis(table, (jnp.arange(top)[None, :] + offset_by) % top, axis=1)


def portions_of(number_of, total, limit, slope, full):
    weights = [(1 << 20) // math.isqrt(grade ** slope) + 1 for grade in range(1, number_of + 1)]
    largest = limit if full else min(limit, max(-(-total // number_of), total * weights[0] // sum(weights)))
    least = 1 if total - largest >= number_of - 1 else 0
    given, spare = [largest] + [least] * (number_of - 1), total - largest - least * (number_of - 1)
    while spare > 0:
        candidates = [i for i in range(1, number_of) if given[i] < largest] or [i for i in range(1, number_of) if given[i] < limit]
        whole, budget = sum([weights[i] for i in candidates]), spare
        for i in candidates:
            addition = min(limit - given[i], max(1, budget * weights[i] // whole), spare)
            given[i] = given[i] + addition
            spare = spare - addition
    return np.array(given)


def bell_draw(rng, extent, scale, limit, cuts=(), held_as=jnp.bfloat16):
    values = jax.random.normal(rng, extent, jnp.float32) * scale
    if len(cuts) > 0:
        values = steps_of(rng, extent, cuts, -0.22, 0.18) * values
    return jnp.clip(values, min=-limit, max=limit).astype(held_as)


def setup_inputs(seed: int = 0, part: int = 0) -> dict:
    keys = jax.random.split(jax.random.key(seed), 7)
    own_keys = jax.random.split(jax.random.fold_in(keys[6], part), 7)
    tokens = bell_draw(own_keys[0], (TOKENS, D), 1.0, 6.0, ((0, 16),))
    route_ids_keys = jax.random.split(jax.random.fold_in(own_keys[1], 1), TOKENS // TOK_DEV)
    route_ids_turns = jax.random.permutation(jax.random.fold_in(own_keys[1], 3), TOKENS // TOK_DEV)
    route_ids = jax.vmap(lambda own, number: shared_out(jax.random.fold_in(own_keys[1], 2), own, number, TOK_DEV, EXPERTS, TOP, CAP, 2))(route_ids_keys, route_ids_turns).reshape((TOKENS, TOP))
    levels = set_ends(jax.random.randint(own_keys[2], (TOKENS, TOP), 1, 65), jax.random.fold_in(own_keys[2], 1), 1, 64).astype(jnp.int32)
    w_gate = bell_draw(keys[3], (N_EXPERT, D, FF_DEV), D ** -0.5, 0.0625, ((0, 16),))
    w_up = bell_draw(keys[4], (N_EXPERT, D, FF_DEV), D ** -0.5, 0.0625, ((0, 16),))
    w_down = bell_draw(keys[5], (N_EXPERT, FF_DEV, D), FF_WIN ** -0.5, 0.125, ((0, 16),))
    return {"tokens": tokens, "route_ids": route_ids, "levels": levels, "w_gate": w_gate, "w_up": w_up, "w_down": w_down}


def reference(tokens, route_ids, levels, w_gate, w_up, w_down):
    total, width = tokens.shape
    top = route_ids.shape[1]
    experts = w_gate.shape[0] // SHARDS
    room = N_EXPERT * CAP
    flat_ids = route_ids.reshape(-1)
    count = flat_ids.shape[0]
    level_f = levels.astype(jnp.float32)
    weights = level_f / jnp.sum(level_f, axis=1, keepdims=True)
    flat_w = weights.reshape(-1)
    padded = jnp.concatenate([tokens, jnp.zeros((1, width), tokens.dtype)], axis=0)
    source = (jnp.arange(count, dtype=jnp.int32) // top).astype(jnp.int32)
    gates = w_gate.reshape(experts, SHARDS, width, FF_DEV)
    ups = w_up.reshape(experts, SHARDS, width, FF_DEV)
    downs = w_down.reshape(experts, SHARDS, FF_DEV, width)

    def one_expert(carry, index):
        chosen = flat_ids == index
        rank = (jnp.cumsum(chosen.astype(jnp.int32)) - 1).astype(jnp.int32)
        place = jnp.where(chosen, rank, room).astype(jnp.int32)
        owner = jnp.full((room,), total, jnp.int32).at[place].set(source, mode="drop")
        rows = padded[owner]
        summed = jnp.zeros((room, width), jnp.float32)
        for shard in range(SHARDS):
            gate = jnp.dot(rows, gates[index, shard], preferred_element_type=jnp.float32)
            up = jnp.dot(rows, ups[index, shard], preferred_element_type=jnp.float32)
            hidden = (jax.nn.silu(gate) * up).astype(jnp.bfloat16)
            part = jnp.dot(hidden, downs[index, shard], preferred_element_type=jnp.float32).astype(jnp.bfloat16)
            part = lax.optimization_barrier(part)
            summed = summed + part.astype(jnp.float32)
        rounded = summed.astype(jnp.bfloat16)
        rounded = lax.optimization_barrier(rounded)
        out_e = rounded.astype(jnp.float32)
        safe = jnp.clip(rank, 0, room - 1).astype(jnp.int32)
        picked = out_e[safe] * jnp.where(chosen, flat_w, jnp.float32(0.0))[:, None]
        return carry + jnp.sum(picked.reshape(total, top, width), axis=1), None

    start = jnp.zeros((total, width), jnp.float32)
    result, unused = lax.scan(one_expert, start, jnp.arange(experts, dtype=jnp.int32))
    return result.astype(jnp.bfloat16)
```

```python
import functools

import jax
import jax.numpy as jnp
from jax import lax
from jax.experimental import pallas as pl
from jax.experimental.pallas import tpu as pltpu
from jax.sharding import PartitionSpec as P

SHARDS = 4
MESH = pl.DeviceIdType.MESH


def tile_of(length, most):
    size = most
    while length % size:
        size //= 2
    return size


def layer_kernel(
    planes, out_ref, gate_hbm, up_hbm, down_hbm, ret_ref,
    x, gate, up, down, acc, hidden, pair, cross,
    w_sem, z_send, z_recv, y_send, y_recv, p_send, p_recv,
    rp_send, rp_recv, ry_send, ry_recv, rz_send, rz_recv,
):
    me = lax.axis_index("expert")
    plane, s = me // SHARDS, me % SHARDS
    base = plane * SHARDS
    core, row = s % 2, s // 2
    partner_s = row * 2 + (1 - core)
    cross_s = (1 - row) * 2 + core
    diag_s = (1 - row) * 2 + (1 - core)
    partner, neighbour = base + partner_s, base + cross_s
    cap, width = x.shape[2], x.shape[3]
    ff = gate.shape[1]
    rows = SHARDS * cap

    barrier = pltpu.get_barrier_semaphore()
    peers = [partner, neighbour]
    peers += [((plane + j) % planes) * SHARDS + s for j in range(1, planes)]
    for peer in peers:
        pl.semaphore_signal(barrier, inc=1, device_id={"expert": peer}, device_id_type=MESH)
    pl.semaphore_wait(barrier, planes + 1)

    def remote(src, dst, send, recv, device):
        return pltpu.make_async_remote_copy(
            src_ref=src, dst_ref=dst, send_sem=send, recv_sem=recv,
            device_id={"expert": device}, device_id_type=MESH,
        )

    def out_copy(j):
        to = (plane + j) % planes
        return remote(out_ref.at[to], x.at[j, s], z_send.at[j], z_recv.at[j], to * SHARDS + s)

    def own_copy():
        return pltpu.make_async_copy(out_ref.at[plane], x.at[0, s], z_recv.at[0])

    def y_copy(j):
        return remote(x.at[j, s], x.at[j, s], y_send.at[j], y_recv.at[j], neighbour)

    def y_arrival(j):
        return remote(x.at[j, cross_s], x.at[j, cross_s], y_send.at[j], y_recv.at[j], neighbour)

    def p_copy(j, k, slot):
        return remote(x.at[j, slot], x.at[j, slot], p_send.at[j, k], p_recv.at[j, k], partner)

    def rp_copy(j, k, slot):
        return remote(x.at[j, slot], pair.at[j, k], rp_send.at[j, k], rp_recv.at[j, k], partner)

    def ry_copy(j):
        return remote(x.at[j, cross_s], cross.at[j], ry_send.at[j], ry_recv.at[j], neighbour)

    def rz_copy(j):
        to = (plane - j + planes) % planes
        return remote(x.at[j, s], ret_ref.at[plane], rz_send.at[j], rz_recv.at[j], to * SHARDS + s)

    own_copy().start()
    for j in range(1, planes):
        out_copy(j).start()
    loads = [
        pltpu.make_async_copy(gate_hbm.at[0], gate, w_sem.at[0]),
        pltpu.make_async_copy(up_hbm.at[0], up, w_sem.at[1]),
        pltpu.make_async_copy(down_hbm.at[0], down, w_sem.at[2]),
    ]
    for load in loads:
        load.start()

    def pass_on(j):
        y_copy(j).start()
        p_copy(j, 0, s).start()

    def finish(j):
        ry_copy(j).wait_recv()
        tile = tile_of(width, 1024)

        @pl.loop(0, width // tile)
        def _(n):
            cols = pl.ds(pl.multiple_of(n * tile, tile), tile)
            total = x[j, s, :, cols].astype(jnp.float32) + pair[j, row, :, cols].astype(jnp.float32)
            x[j, s, :, cols] = (total + cross[j, :, cols].astype(jnp.float32)).astype(x.dtype)

        @pl.when(j > 0)
        def _():
            rz_copy(j).start()

        @pl.when(j == 0)
        def _():
            pltpu.make_async_copy(x.at[0, s], ret_ref.at[plane], rz_send.at[0]).start()

    own_copy().wait()
    pass_on(0)

    @pl.loop(0, planes)
    def _(j):
        @pl.when(j + 1 < planes)
        def _():
            out_copy(j + 1).wait_recv()
            pass_on(j + 1)

        y_arrival(j).wait_recv()
        p_copy(j, 1, cross_s).start()
        p_copy(j, 0, partner_s).wait_recv()
        p_copy(j, 1, diag_s).wait_recv()

        @pl.when(j == 0)
        def _():
            for load in loads:
                load.wait()

        acc[...] = jnp.zeros_like(acc)
        k_tile = tile_of(width, 1024)

        @pl.loop(0, width // k_tile)
        def _(k):
            cols = pl.ds(pl.multiple_of(k * k_tile, k_tile), k_tile)
            part = x[j, :, :, cols].reshape(rows, k_tile)
            acc[0] += jnp.dot(part, gate[cols, :], preferred_element_type=jnp.float32)
            acc[1] += jnp.dot(part, up[cols, :], preferred_element_type=jnp.float32)

        value = acc[0]
        hidden[...] = (value / (1.0 + jnp.exp(-value)) * acc[1]).astype(hidden.dtype)

        y_copy(j).wait_send()
        p_copy(j, 0, s).wait_send()
        p_copy(j, 1, cross_s).wait_send()
        n_tile = tile_of(width, 512)

        @pl.loop(0, width // n_tile)
        def _(n):
            cols = pl.ds(pl.multiple_of(n * n_tile, n_tile), n_tile)
            part = jnp.dot(hidden[...], down[:, cols], preferred_element_type=jnp.float32)
            x[j, :, :, cols] = part.astype(x.dtype).reshape(SHARDS, cap, n_tile)

        rp_copy(j, 1 - row, diag_s).start()
        rp_copy(j, row, partner_s).start()
        rp_copy(j, 1 - row, diag_s).wait_recv()
        rp_copy(j, row, partner_s).wait_recv()
        tile = tile_of(width, 1024)

        @pl.loop(0, width // tile)
        def _(n):
            cols = pl.ds(pl.multiple_of(n * tile, tile), tile)
            total = x[j, cross_s, :, cols].astype(jnp.float32) + pair[j, 1 - row, :, cols].astype(jnp.float32)
            x[j, cross_s, :, cols] = total.astype(x.dtype)

        ry_copy(j).start()

        @pl.when(j > 0)
        def _():
            finish(j - 1)

    finish(planes - 1)
    for j in range(planes):
        rp_copy(j, 1 - row, diag_s).wait_send()
        rp_copy(j, row, partner_s).wait_send()
        ry_copy(j).wait_send()
    pltpu.make_async_copy(x.at[0, s], ret_ref.at[plane], rz_send.at[0]).wait()
    for j in range(1, planes):
        out_copy(j).wait_send()
        rz_copy(j).wait()


def combine_kernel(weight_ref, ret_ref, out_ref):
    weight = weight_ref[...]
    high = weight.astype(jnp.bfloat16)
    low = (weight - high.astype(jnp.float32)).astype(jnp.bfloat16)
    total = jnp.dot(high, ret_ref[...], preferred_element_type=jnp.float32)
    total += jnp.dot(low, ret_ref[...], preferred_element_type=jnp.float32)
    out_ref[...] = total.astype(out_ref.dtype)


def on_device(tokens, route_ids, levels, w_gate, w_up, w_down):
    tok_rows, width = tokens.shape
    top = route_ids.shape[1]
    ff = w_gate.shape[2]
    experts = lax.axis_size("expert") // SHARDS
    capacity = 5 * tok_rows * top // (4 * experts)
    cap = -(-capacity // 16) * 16
    slots = experts * cap
    dtype = tokens.dtype

    chosen = route_ids[:, :, None] == jnp.arange(experts, dtype=jnp.int32)
    named = jnp.any(chosen, axis=1)
    index = jnp.arange(tok_rows, dtype=jnp.int32)
    earlier = (index[:, None] > index[None, :]).astype(jnp.bfloat16)
    rank = jnp.dot(earlier, named.astype(jnp.bfloat16), preferred_element_type=jnp.float32)
    place = jnp.where(named, rank.astype(jnp.int32), cap)
    level_f = levels.astype(jnp.float32)
    weights = level_f / jnp.sum(level_f, axis=1, keepdims=True)
    weight_e = jnp.sum(jnp.where(chosen, weights[:, :, None], 0.0), axis=1)
    spot = jnp.arange(cap, dtype=jnp.int32)
    pick = (place[:, :, None] == spot).reshape(tok_rows, slots)
    weight_m = jnp.where(pick, jnp.repeat(weight_e, cap, axis=1), 0.0)
    outgoing = lax.dot_general(
        pick.astype(dtype), tokens, (((0,), (0,)), ((), ())), preferred_element_type=jnp.float32
    ).astype(dtype).reshape(experts, cap, width)

    dma, anywhere = pltpu.SemaphoreType.DMA, pl.BlockSpec(memory_space=pl.ANY)
    rows = SHARDS * cap
    returned = pl.pallas_call(
        functools.partial(layer_kernel, experts),
        out_shape=jax.ShapeDtypeStruct((experts, cap, width), dtype),
        in_specs=[anywhere] * 4,
        out_specs=anywhere,
        scratch_shapes=[
            pltpu.VMEM((experts, SHARDS, cap, width), dtype),
            pltpu.VMEM((width, ff), dtype),
            pltpu.VMEM((width, ff), dtype),
            pltpu.VMEM((ff, width), dtype),
            pltpu.VMEM((2, rows, ff), jnp.float32),
            pltpu.VMEM((rows, ff), dtype),
            pltpu.VMEM((experts, 2, cap, width), dtype),
            pltpu.VMEM((experts, cap, width), dtype),
            dma((3,)),
            dma((experts,)), dma((experts,)),
            dma((experts,)), dma((experts,)),
            dma((experts, 2)), dma((experts, 2)),
            dma((experts, 2)), dma((experts, 2)),
            dma((experts,)), dma((experts,)),
            dma((experts,)), dma((experts,)),
        ],
        compiler_params=pltpu.CompilerParams(
            collective_id=0, has_side_effects=True, vmem_limit_bytes=67_000_000
        ),
    )(outgoing, w_gate, w_up, w_down)

    tile = tile_of(width, 1024)
    return pl.pallas_call(
        combine_kernel,
        out_shape=jax.ShapeDtypeStruct((tok_rows, width), dtype),
        grid=(width // tile,),
        in_specs=[
            pl.BlockSpec((tok_rows, slots), lambda n: (0, 0)),
            pl.BlockSpec((slots, tile), lambda n: (0, n)),
        ],
        out_specs=pl.BlockSpec((tok_rows, tile), lambda n: (0, n)),
    )(weight_m, returned.reshape(slots, width))


def solution(mesh):
    return jax.shard_map(
        on_device,
        mesh=mesh,
        in_specs=(
            P(("groups", "expert"), None),
            P(("groups", "expert"), None),
            P(("groups", "expert"), None),
            P("expert", None, None),
            P("expert", None, None),
            P("expert", None, None),
        ),
        out_specs=P(("groups", "expert"), None),
        check_vma=False,
    )
```

```python
import functools

import jax
import jax.numpy as jnp
from jax import lax
from jax.experimental import pallas as pl
from jax.experimental.pallas import tpu as pltpu
from jax.sharding import PartitionSpec as P

SHARDS = 4
MESH = pl.DeviceIdType.MESH


def tile_of(length, most):
    size = most
    while length % size:
        size //= 2
    return size


def xor(a, mask, count):
    total, bit = 0, 1
    while bit < count:
        total += (a // bit + mask // bit) % 2 * bit
        bit *= 2
    return total


def layer_kernel(
    planes, out_ref, gate_hbm, up_hbm, down_hbm, ret_ref,
    x, gate, up, down, acc, hidden, pair, cross,
    w_sem, z_send, z_recv, y_send, y_recv, p_send, p_recv,
    rp_send, rp_recv, ry_send, ry_recv, rz_send, rz_recv,
):
    me = lax.axis_index("expert")
    plane, s = me // SHARDS, me % SHARDS
    base = plane * SHARDS
    core, row = s % 2, s // 2
    partner_s = row * 2 + (1 - core)
    cross_s = (1 - row) * 2 + core
    diag_s = (1 - row) * 2 + (1 - core)
    partner, neighbour = base + partner_s, base + cross_s
    cap, width = x.shape[2], x.shape[3]
    rows = SHARDS * cap
    tile = tile_of(width, 1024)
    chunks = width // tile

    barrier = pltpu.get_barrier_semaphore()
    peers = [partner, neighbour]
    peers += [xor(plane, j, planes) * SHARDS + s for j in range(1, planes)]
    for peer in peers:
        pl.semaphore_signal(barrier, inc=1, device_id={"expert": peer}, device_id_type=MESH)
    pl.semaphore_wait(barrier, planes + 1)

    def remote(src, dst, send, recv, device):
        return pltpu.make_async_remote_copy(
            src_ref=src, dst_ref=dst, send_sem=send, recv_sem=recv,
            device_id={"expert": device}, device_id_type=MESH,
        )

    def columns(q):
        return pl.ds(pl.multiple_of(q * tile, tile), tile)

    def out_copy(j):
        to = xor(plane, j, planes)
        return remote(out_ref.at[to], x.at[j, s], z_send.at[j], z_recv.at[j], to * SHARDS + s)

    def own_copy():
        return pltpu.make_async_copy(out_ref.at[plane], x.at[0, s], z_recv.at[0])

    def y_copy(j):
        return remote(x.at[j, s], x.at[j, s], y_send.at[j], y_recv.at[j], neighbour)

    def y_arrival(j):
        return remote(x.at[j, cross_s], x.at[j, cross_s], y_send.at[j], y_recv.at[j], neighbour)

    def p_copy(j, k, slot):
        return remote(x.at[j, slot], x.at[j, slot], p_send.at[j, k], p_recv.at[j, k], partner)

    def rp_copy(j, q, k, slot):
        cols = columns(q)
        return remote(
            x.at[j, slot, :, cols], pair.at[j, k, :, cols],
            rp_send.at[j, q, k], rp_recv.at[j, q, k], partner,
        )

    def ry_copy(j, q):
        cols = columns(q)
        return remote(
            x.at[j, cross_s, :, cols], cross.at[j, :, cols],
            ry_send.at[j, q], ry_recv.at[j, q], neighbour,
        )

    def rz_copy(j, q):
        cols, to = columns(q), xor(plane, j, planes)
        return remote(
            x.at[j, s, :, cols], ret_ref.at[plane, :, cols],
            rz_send.at[j, q], rz_recv.at[j, q], to * SHARDS + s,
        )

    def keep_copy(q):
        cols = columns(q)
        return pltpu.make_async_copy(x.at[0, s, :, cols], ret_ref.at[plane, :, cols], rz_send.at[0, q])

    own_copy().start()
    for distance in range(1, planes):
        for to in (plane + distance, plane - distance):
            @pl.when((to >= 0) & (to < planes))
            def _():
                mask = xor(plane, to, planes)
                remote(
                    out_ref.at[to], x.at[mask, s], z_send.at[mask], z_recv.at[mask], to * SHARDS + s
                ).start()
    loads = [
        pltpu.make_async_copy(gate_hbm.at[0], gate, w_sem.at[0]),
        pltpu.make_async_copy(up_hbm.at[0], up, w_sem.at[1]),
        pltpu.make_async_copy(down_hbm.at[0], down, w_sem.at[2]),
    ]
    for load in loads:
        load.start()

    def arrive(j):
        if j == 0:
            own_copy().wait()
        else:
            out_copy(j).wait_recv()
        y_copy(j).start()
        p_copy(j, 0, s).start()

    def gather(j):
        y_arrival(j).wait_recv()
        p_copy(j, 1, cross_s).start()
        p_copy(j, 0, partner_s).wait_recv()
        p_copy(j, 1, diag_s).wait_recv()

    def expand(j):
        @pl.loop(0, chunks)
        def _(q):
            cols = columns(q)
            part = x[j, :, :, cols].reshape(rows, tile)

            @pl.when(q == 0)
            def _():
                acc[...] = jnp.zeros_like(acc)

            acc[0] += jnp.dot(part, gate[cols, :], preferred_element_type=jnp.float32)
            acc[1] += jnp.dot(part, up[cols, :], preferred_element_type=jnp.float32)

        value = acc[0]
        hidden[...] = (value / (1.0 + jnp.exp(-value)) * acc[1]).astype(hidden.dtype)

    def contract(j):
        y_copy(j).wait_send()
        p_copy(j, 0, s).wait_send()
        p_copy(j, 1, cross_s).wait_send()

        @pl.loop(0, chunks + 1)
        def _(q):
            @pl.when(q < chunks)
            def _():
                cols = columns(q)
                part = jnp.dot(hidden[...], down[:, cols], preferred_element_type=jnp.float32)
                x[j, :, :, cols] = part.astype(x.dtype).reshape(SHARDS, cap, tile)
                rp_copy(j, q, 1 - row, diag_s).start()
                rp_copy(j, q, row, partner_s).start()

            @pl.when(q > 0)
            def _():
                cols = columns(q - 1)
                rp_copy(j, q - 1, 1 - row, diag_s).wait_recv()
                total = x[j, cross_s, :, cols].astype(jnp.float32)
                total += pair[j, 1 - row, :, cols].astype(jnp.float32)
                x[j, cross_s, :, cols] = total.astype(x.dtype)
                ry_copy(j, q - 1).start()

    def finish(j):
        @pl.loop(0, chunks)
        def _(q):
            cols = columns(q)
            rp_copy(j, q, row, partner_s).wait_recv()
            total = x[j, s, :, cols].astype(jnp.float32) + pair[j, row, :, cols].astype(jnp.float32)
            ry_copy(j, q).wait_recv()
            x[j, s, :, cols] = (total + cross[j, :, cols].astype(jnp.float32)).astype(x.dtype)
            if j > 0:
                rz_copy(j, q).start()
            else:
                keep_copy(q).start()

    order = [0, *range(2, planes), 1]
    arrive(0)
    arrive(1)
    for i, j in enumerate(order):
        gather(j)
        if 0 < i < planes - 2:
            arrive(order[i + 1])
        if i == 0:
            for load in loads:
                load.wait()
        expand(j)
        contract(j)
        if i == 0:
            arrive(order[1])
        else:
            finish(order[i - 1])
    finish(order[-1])

    for j in range(planes):
        @pl.loop(0, chunks)
        def _(q):
            rp_copy(j, q, 1 - row, diag_s).wait_send()
            rp_copy(j, q, row, partner_s).wait_send()
            ry_copy(j, q).wait_send()
            if j > 0:
                rz_copy(j, q).wait()
            else:
                keep_copy(q).wait()
        if j > 0:
            out_copy(j).wait_send()


def combine_kernel(weight_ref, ret_ref, out_ref):
    weight = weight_ref[...]
    high = weight.astype(jnp.bfloat16)
    low = (weight - high.astype(jnp.float32)).astype(jnp.bfloat16)
    total = jnp.dot(high, ret_ref[...], preferred_element_type=jnp.float32)
    total += jnp.dot(low, ret_ref[...], preferred_element_type=jnp.float32)
    out_ref[...] = total.astype(out_ref.dtype)


def on_device(tokens, route_ids, levels, w_gate, w_up, w_down):
    tok_rows, width = tokens.shape
    top = route_ids.shape[1]
    ff = w_gate.shape[2]
    experts = lax.axis_size("expert") // SHARDS
    capacity = 5 * tok_rows * top // (4 * experts)
    cap = -(-capacity // 16) * 16
    slots = experts * cap
    dtype = tokens.dtype

    chosen = route_ids[:, :, None] == jnp.arange(experts, dtype=jnp.int32)
    named = jnp.any(chosen, axis=1)
    index = jnp.arange(tok_rows, dtype=jnp.int32)
    earlier = (index[:, None] > index[None, :]).astype(jnp.bfloat16)
    rank = jnp.dot(earlier, named.astype(jnp.bfloat16), preferred_element_type=jnp.float32)
    place = jnp.where(named, rank.astype(jnp.int32), cap)
    level_f = levels.astype(jnp.float32)
    weights = level_f / jnp.sum(level_f, axis=1, keepdims=True)
    weight_e = jnp.sum(jnp.where(chosen, weights[:, :, None], 0.0), axis=1)
    spot = jnp.arange(cap, dtype=jnp.int32)
    pick = (place[:, :, None] == spot).reshape(tok_rows, slots)
    weight_m = jnp.where(pick, jnp.repeat(weight_e, cap, axis=1), 0.0)
    outgoing = lax.dot_general(
        pick.astype(dtype), tokens, (((0,), (0,)), ((), ())), preferred_element_type=jnp.float32
    ).astype(dtype).reshape(experts, cap, width)

    dma, anywhere = pltpu.SemaphoreType.DMA, pl.BlockSpec(memory_space=pl.ANY)
    rows, chunks = SHARDS * cap, width // tile_of(width, 1024)
    returned = pl.pallas_call(
        functools.partial(layer_kernel, experts),
        out_shape=jax.ShapeDtypeStruct((experts, cap, width), dtype),
        in_specs=[anywhere] * 4,
        out_specs=anywhere,
        scratch_shapes=[
            pltpu.VMEM((experts, SHARDS, cap, width), dtype),
            pltpu.VMEM((width, ff), dtype),
            pltpu.VMEM((width, ff), dtype),
            pltpu.VMEM((ff, width), dtype),
            pltpu.VMEM((2, rows, ff), jnp.float32),
            pltpu.VMEM((rows, ff), dtype),
            pltpu.VMEM((experts, 2, cap, width), dtype),
            pltpu.VMEM((experts, cap, width), dtype),
            dma((3,)),
            dma((experts,)), dma((experts,)),
            dma((experts,)), dma((experts,)),
            dma((experts, 2)), dma((experts, 2)),
            dma((experts, chunks, 2)), dma((experts, chunks, 2)),
            dma((experts, chunks)), dma((experts, chunks)),
            dma((experts, chunks)), dma((experts, chunks)),
        ],
        compiler_params=pltpu.CompilerParams(
            collective_id=0, has_side_effects=True, vmem_limit_bytes=67_000_000
        ),
    )(outgoing, w_gate, w_up, w_down)

    tile = tile_of(width, 1024)
    return pl.pallas_call(
        combine_kernel,
        out_shape=jax.ShapeDtypeStruct((tok_rows, width), dtype),
        grid=(width // tile,),
        in_specs=[
            pl.BlockSpec((tok_rows, slots), lambda n: (0, 0)),
            pl.BlockSpec((slots, tile), lambda n: (0, n)),
        ],
        out_specs=pl.BlockSpec((tok_rows, tile), lambda n: (0, n)),
    )(weight_m, returned.reshape(slots, width))


def solution(mesh):
    return jax.shard_map(
        on_device,
        mesh=mesh,
        in_specs=(
            P(("groups", "expert"), None),
            P(("groups", "expert"), None),
            P(("groups", "expert"), None),
            P("expert", None, None),
            P("expert", None, None),
            P("expert", None, None),
        ),
        out_specs=P(("groups", "expert"), None),
        check_vma=False,
    )
```
